32 devices in a mesh: doc: 2 (over x), seq: 4 (over y, core), head: 4 (over z).
Axes of the slice: x: 2, y: 2, z: 4, core: 2. Of those that a mesh axis runs over, the one named last changes fastest.
Arguments:
- length: int32 [2], P('doc'), parts along dimension 0, may hold values from 896 to 1024
- residual: bfloat16 [2048, 4096], P(('doc', 'seq'), 'head'), parts along dimension 0, may hold values from -6 to 6
- ssm_input: bfloat16 [2048, 4096], P(('doc', 'seq'), 'head'), parts along dimension 0, may hold values from -6 to 6
- state_in: bfloat16 [2048, 128], P(('doc', 'seq')), parts along dimension 0, may hold values from -6 to 6
- state_out: bfloat16 [2048, 128], P(('doc', 'seq')), parts along dimension 0, may hold values from -0.5 to 0.5
- step_raw: float32 [128, 1024], P(('doc', 'head'), 'seq'), parts along dimension 0, may hold values from -5 to 2
- decay_rate: float32 [64], P('head'), may hold values from 0 to 1, as said below
- ssm_gain: float32 [4096], P('head'), may hold values from 0.1 to 1.9
- out_weight: bfloat16 [4096, 4096], P('head'), may hold values from -0.09375 to 0.09375
- norm_gain: float32 [4096], replicated, may hold values from 0.1 to 1.9
- query_weight: bfloat16 [4096, 4096], P(None, 'head'), may hold values from -2 to 2
- key_weight: bfloat16 [4096, 1024], P(None, 'head'), may hold values from -3 to 3
- value_weight: bfloat16 [4096, 1024], P(None, 'head'), may hold values from -0.09375 to 0.09375
Outputs:
- layer_out: bfloat16 [2048, 4096], P(('doc', 'seq'), 'head'), parts along dimension 0
- head_out: bfloat16 [2048, 4096], P(('doc', 'seq'), 'head'), parts along dimension 0
The draws below stay inside these ranges and needn't reach their ends.
There are 2 independent parts, one for each index of `doc`. The reference program is written for one: setup_inputs(seed, part) draws one part's arguments, and reference() takes and returns one part's arrays. A program takes and returns all parts, laid end to end along the dimension named above; an argument that names none is the same for every part. Nothing has to cross between parts.
Inputs may be any that keep to these rules, and one draw needn't show every extreme that they name: The document fills positions 0 to length - 1 of the 1024; later positions are padding. `decay_rate`: positive.
All inputs are finite; a program needn't handle non-finite values.
Results may differ from the reference program's by a relative error of at most 0.028.
The reference program's roundings to bfloat16 on the way count: a program that leaves them out, or rounds other values in their place, can miss the bound.
Values may be sent and summed in bfloat16 or wider, within the bound.
A program may use at most 64 MiB of HBM per device.

```python
import jax
import jax.numpy as jnp
from jax import lax

D = 4096
SSM_HEADS = 64
SSM_HDIM = 64
STATE = 128
Q_HEADS = 32
KV_HEADS = 8
HEAD_DIM = 128
TOK_DEV = 256
INNER = 4096
TOKENS = 1024


def draw_step_raw(key, part):
    blocks = TOKENS // TOK_DEV
    base = jax.random.uniform(jax.random.fold_in(key, 31), (SSM_HEADS, blocks, TOK_DEV), jnp.float32, -3.5, 1.0)
    offset = jax.random.uniform(jax.random.fold_in(key, 32), (SSM_HEADS, blocks, 1), jnp.float32, -1.5, 1.0)
    return (base + offset).reshape(SSM_HEADS, TOKENS)


def draw_decay_rate(key, part):
    order = jax.random.permutation(jax.random.fold_in(key, 21), SSM_HEADS)
    slow = order < SSM_HEADS // 2
    spread = jax.random.uniform(jax.random.fold_in(key, 22), (SSM_HEADS,), jnp.float32)
    slow_rate = jnp.exp(jnp.log(0.25 / TOKENS) + spread * jnp.log(12.0))
    fast_rate = jnp.exp(jnp.log(0.05) + spread * jnp.log(20.0))
    return jnp.where(slow, slow_rate, fast_rate)


def query_key_pair(key):
    scale = 1.6 * D ** (-0.5)
    query_part = jnp.clip(jax.random.normal(jax.random.fold_in(key, 11), (D, Q_HEADS * HEAD_DIM), jnp.float32), -6.0, 6.0) * scale
    key_part = jnp.clip(jax.random.normal(jax.random.fold_in(key, 12), (D, KV_HEADS * HEAD_DIM), jnp.float32), -6.0, 6.0) * scale
    return (query_part, key_part)


def draw_query_weight(key, part):
    return query_key_pair(key)[0].astype(jnp.bfloat16)


def draw_key_weight(key, part):
    return query_key_pair(key)[1].astype(jnp.bfloat16)


def levels(stream_key, extent, split, smallest, top_value):
    gain, own = 1.0, jax.random.fold_in(stream_key, 6)
    for dim, blocks in split:
        heights = jnp.exp(jax.random.uniform(jax.random.fold_in(own, dim), (blocks,), jnp.float32, smallest / len(split), top_value / len(split)))
        gain = gain * jnp.repeat(heights, extent[dim] // blocks).reshape([-1 if axis == dim else 1 for axis in range(len(extent))])
    return gain


def centred(rng, extent, scale, reach, shards=(), kind=jnp.bfloat16):
    drawn = scale * jax.random.normal(rng, extent, jnp.float32)
    if shards:
        drawn = drawn * levels(rng, extent, shards, -0.22, 0.18)
    return jnp.clip(drawn, -reach, reach).astype(kind)


def setup_inputs(seed: int = 0, part: int = 0) -> dict:
    key_list = jax.random.split(jax.random.key(seed), 14)
    part_keys = jax.random.split(jax.random.fold_in(key_list[13], part), 14)
    length = jax.random.randint(part_keys[0], (1,), TOKENS - TOK_DEV // 2, TOKENS + 1).astype(jnp.int32)
    residual = centred(part_keys[1], (TOKENS, D), 1.0, 6.0, ((0, 4), (1, 4)))
    ssm_input = centred(part_keys[2], (TOKENS, INNER), 1.0, 6.0, ((0, 4), (1, 4)))
    state_in = centred(part_keys[3], (TOKENS, STATE), 1.0, 6.0, ((0, 4),))
    state_out = centred(part_keys[4], (TOKENS, STATE), STATE ** -0.5, 0.5, ((0, 4),))
    step_raw = draw_step_raw(jax.random.fold_in(jax.random.fold_in(key_list[13], part), 71), part)
    decay_rate = draw_decay_rate(jax.random.fold_in(key_list[13], 71), part)
    ssm_gain = jnp.clip(1.0 + 0.18 * jax.random.normal(key_list[7], (INNER,), jnp.float32), 0.1, 1.9)
    out_weight = centred(key_list[8], (INNER, D), INNER ** -0.5, 0.09375, ((0, 4),))
    norm_gain = jnp.clip(1.0 + 0.18 * jax.random.normal(key_list[9], (D,), jnp.float32), 0.1, 1.9)
    query_weight = draw_query_weight(jax.random.fold_in(key_list[13], 71), part)
    key_weight = draw_key_weight(jax.random.fold_in(key_list[13], 71), part)
    value_weight = centred(key_list[12], (D, KV_HEADS * HEAD_DIM), D ** -0.5, 0.09375, ((1, 4),))
    return dict(length=length, residual=residual, ssm_input=ssm_input, state_in=state_in, state_out=state_out, step_raw=step_raw, decay_rate=decay_rate, ssm_gain=ssm_gain, out_weight=out_weight, norm_gain=norm_gain, query_weight=query_weight, key_weight=key_weight, value_weight=value_weight)


EPSILON = 1e-05
NEG_BIG = -1e+30
HIGHEST = lax.Precision.HIGHEST

def ssd_blocks(ssm_input, state_in, state_out, delta, decay_rate):
    blocks = TOKENS // TOK_DEV
    inputs = ssm_input.astype(jnp.float32).reshape(blocks, TOK_DEV, SSM_HEADS, SSM_HDIM)
    enter = state_in.reshape(blocks, TOK_DEV, STATE)
    leave = state_out.reshape(blocks, TOK_DEV, STATE)
    steps = delta.reshape(SSM_HEADS, blocks, TOK_DEV).transpose(1, 0, 2)
    causal = jnp.arange(TOK_DEV)[:, None] >= jnp.arange(TOK_DEV)[None, :]

    def advance(carried, inputs_now):
        block_in, enter_now, leave_now, step_now = inputs_now
        cumlog = jnp.cumsum(-decay_rate[:, None] * step_now, axis=1)
        inner = jnp.dot(leave_now, enter_now.T, preferred_element_type=jnp.float32)
        spread = cumlog[:, :, None] - cumlog[:, None, :]
        mixing = jnp.where(causal[None], jnp.exp(jnp.where(causal[None], spread, 0.0)), 0.0) * inner[None] * step_now[:, None, :]
        within = jnp.einsum('hts,shp->thp', mixing, block_in, precision=HIGHEST)
        carried_out = jnp.einsum('hpn,tn->thp', carried, leave_now.astype(jnp.float32), precision=HIGHEST)
        output = within + jnp.exp(cumlog).T[:, :, None] * carried_out
        tail = jnp.exp(cumlog[:, -1:] - cumlog) * step_now
        fresh = jnp.einsum('hs,shp,sn->hpn', tail, block_in, enter_now.astype(jnp.float32), precision=HIGHEST)
        following = jnp.exp(cumlog[:, -1])[:, None, None] * carried + fresh
        return (following, output)
    start = jnp.zeros((SSM_HEADS, SSM_HDIM, STATE), jnp.float32)
    unused, outputs = lax.scan(advance, start, (inputs, enter, leave, steps))
    return outputs.reshape(TOKENS, SSM_HEADS, SSM_HDIM)

def reference(length, residual, ssm_input, state_in, state_out, step_raw, decay_rate, ssm_gain, out_weight, norm_gain, query_weight, key_weight, value_weight):
    positions = jnp.arange(TOKENS, dtype=jnp.int32)
    live_rows = positions < length[0]
    live = live_rows.astype(jnp.float32)
    delta = live[None, :] * jax.nn.softplus(step_raw)
    ssm_out = ssd_blocks(ssm_input, state_in, state_out, delta, decay_rate) * live[:, None, None]
    mean_square = lax.optimization_barrier(jnp.mean(ssm_out * ssm_out, axis=2, keepdims=True))
    normed = (ssm_out * lax.rsqrt(mean_square + EPSILON) * ssm_gain.reshape(SSM_HEADS, SSM_HDIM)).astype(jnp.bfloat16)
    normed = normed.reshape(TOKENS, SSM_HEADS * SSM_HDIM)
    projected = jnp.dot(normed, out_weight, preferred_element_type=jnp.float32)
    layer_out = (residual.astype(jnp.float32) + projected).astype(jnp.bfloat16)
    widened = layer_out.astype(jnp.float32)
    attn_in = (widened * lax.rsqrt(lax.optimization_barrier(jnp.mean(widened * widened, axis=1, keepdims=True)) + EPSILON) * norm_gain).astype(jnp.bfloat16)
    queries = jnp.dot(attn_in, query_weight, preferred_element_type=jnp.float32).astype(jnp.bfloat16)
    keys = jnp.dot(attn_in, key_weight, preferred_element_type=jnp.float32).astype(jnp.bfloat16)
    values = jnp.dot(attn_in, value_weight, preferred_element_type=jnp.float32).astype(jnp.bfloat16)
    group_size = Q_HEADS // KV_HEADS
    query_heads = queries.reshape(TOKENS, Q_HEADS, HEAD_DIM).transpose(1, 0, 2)
    key_heads = jnp.repeat(keys.reshape(TOKENS, KV_HEADS, HEAD_DIM).transpose(1, 0, 2), group_size, axis=0)
    value_heads = jnp.repeat(values.reshape(TOKENS, KV_HEADS, HEAD_DIM).transpose(1, 0, 2), group_size, axis=0)
    allowed = (positions[None, :] <= positions[:, None]) & live_rows[None, :]

    def one_head(operands):
        query_now, key_now, value_now = operands
        scores = jnp.dot(query_now, key_now.T, preferred_element_type=jnp.float32) * HEAD_DIM ** (-0.5)
        masked = jnp.where(allowed, scores, NEG_BIG)
        best = lax.optimization_barrier(jnp.max(masked, axis=1, keepdims=True))
        weights = jnp.where(allowed, jnp.exp(masked - best), 0.0)
        total = lax.optimization_barrier(jnp.sum(weights, axis=1, keepdims=True))
        mixed = jnp.dot(weights.astype(jnp.bfloat16), value_now, preferred_element_type=jnp.float32)
        return mixed / jnp.where(live_rows[:, None], total, 1.0) * live[:, None]
    heads = lax.map(one_head, (query_heads, key_heads, value_heads))
    head_out = heads.transpose(1, 0, 2).reshape(TOKENS, Q_HEADS * HEAD_DIM).astype(jnp.bfloat16)
    return (layer_out, head_out)
```

```python
import functools

import jax
import jax.numpy as jnp
from jax import lax
from jax.experimental import pallas as pl
from jax.experimental.pallas import tpu as pltpu
from jax.sharding import PartitionSpec as P

HEAD_DIM = 128


EPSILON = 1e-05
NEG_BIG = -1e30
HIGHEST = lax.Precision.HIGHEST


def chain_kernel(
    count, chunks, decay_ref, state_ref, incoming_ref, stage_ref, landed_ref, send_sem, recv_sem
):
    mine = lax.axis_index("seq")
    last = count - 1
    heads = state_ref.shape[0] // chunks
    barrier = pltpu.get_barrier_semaphore()

    def greet(neighbour):
        pl.semaphore_signal(
            barrier, inc=1, device_id={"seq": neighbour}, device_id_type=pl.DeviceIdType.MESH
        )

    @pl.when(mine > 0)
    def _():
        greet(mine - 1)

    @pl.when(mine < last)
    def _():
        greet(mine + 1)

    @pl.when((mine == 0) | (mine == last))
    def _():
        pl.semaphore_wait(barrier, 1)

    @pl.when((mine > 0) & (mine < last))
    def _():
        pl.semaphore_wait(barrier, 2)

    def copy(chunk):
        return pltpu.make_async_remote_copy(
            src_ref=stage_ref.at[chunk],
            dst_ref=landed_ref.at[chunk],
            send_sem=send_sem.at[chunk],
            recv_sem=recv_sem.at[chunk],
            device_id={"seq": mine + 1},
            device_id_type=pl.DeviceIdType.MESH,
        )

    for chunk in range(chunks):
        here = pl.ds(chunk * heads, heads)

        @pl.when(mine == 0)
        def _():
            incoming_ref[here] = jnp.zeros((heads,) + state_ref.shape[1:], jnp.float32)

        @pl.when(mine > 0)
        def _():
            copy(chunk).wait_recv()
            incoming_ref[here] = landed_ref[chunk].astype(jnp.float32)

        @pl.when(mine < last)
        def _():
            for index in range(heads):
                head = chunk * heads + index
                outgoing = decay_ref[head] * incoming_ref[head] + state_ref[head]
                stage_ref[chunk, index] = outgoing.astype(jnp.bfloat16)
            copy(chunk).start()

    for chunk in range(chunks):

        @pl.when(mine < last)
        def _():
            copy(chunk).wait_send()


def incoming_state(block_decay, local_state, count):
    heads, width, states = local_state.shape
    chunks = 4 if heads % 4 == 0 else 1
    slots = (chunks, heads // chunks, width, states)
    return pl.pallas_call(
        functools.partial(chain_kernel, count, chunks),
        out_shape=jax.ShapeDtypeStruct(local_state.shape, jnp.float32),
        in_specs=[
            pl.BlockSpec(memory_space=pltpu.SMEM),
            pl.BlockSpec(memory_space=pltpu.VMEM),
        ],
        out_specs=pl.BlockSpec(memory_space=pltpu.VMEM),
        scratch_shapes=[
            pltpu.VMEM(slots, jnp.bfloat16),
            pltpu.VMEM(slots, jnp.bfloat16),
            pltpu.SemaphoreType.DMA((chunks,)),
            pltpu.SemaphoreType.DMA((chunks,)),
        ],
        compiler_params=pltpu.CompilerParams(collective_id=1, has_side_effects=True),
    )(block_decay, local_state)


def line_kernel(
    count,
    shards,
    chunks,
    lag,
    normed_ref,
    out_weight_ref,
    residual_ref,
    gain_ref,
    query_weight_ref,
    key_weight_ref,
    value_weight_ref,
    layer_ref,
    query_ref,
    key_value_ref,
    block_weight_ref,
    partial_ref,
    weight_ref,
    attn_ref,
    shared_ref,
    stage_ref,
    landed_ref,
    final_ref,
    sum_send,
    sum_recv,
    final_send,
    final_recv,
    shard_send,
    shard_recv,
    weight_sem,
    block_sem,
):
    mine = lax.axis_index("head")
    last = count - 1
    half = count // 2
    left = mine < half
    place = jnp.where(left, mine, last - mine)
    inner = (mine == half - 1) | (mine == half)
    inward = jnp.where(left, mine + 1, mine - 1)
    outward = jnp.where(left, mine - 1, mine + 1)
    inner_slot = inner.astype(jnp.int32)

    pieces, piece_rows, piece_width = stage_ref.shape
    rows, width = residual_ref.shape
    blocks = pieces // chunks
    per_owner = width // piece_width

    shard = lax.axis_index("seq")
    query_width = query_ref.shape[1]
    kv_width = key_weight_ref.shape[1]
    tile = 2 * kv_width
    starts = (0, kv_width, tile)
    loads = [
        pltpu.make_async_copy(
            source, weight_ref.at[:, pl.ds(start, source.shape[1])], weight_sem.at[index]
        )
        for index, (source, start) in enumerate(
            zip((key_weight_ref, value_weight_ref, query_weight_ref), starts)
        )
    ]

    def block_load(block):
        columns = pl.ds(pl.multiple_of(block * piece_width, 128), piece_width)
        return pltpu.make_async_copy(
            out_weight_ref.at[:, columns], block_weight_ref.at[block], block_sem.at[block]
        )

    @pl.loop(0, blocks)
    def _(block):
        block_load(block).start()

    for load in loads:
        load.start()

    barrier = pltpu.get_barrier_semaphore()

    def greet(neighbour):
        pl.semaphore_signal(
            barrier, inc=1, device_id={"head": neighbour}, device_id_type=pl.DeviceIdType.MESH
        )

    @pl.when(mine > 0)
    def _():
        greet(mine - 1)

    @pl.when(mine < last)
    def _():
        greet(mine + 1)

    for offset in range(1, shards):
        other = (shard + offset) % shards
        pl.semaphore_signal(
            barrier, inc=1, device_id={"seq": other}, device_id_type=pl.DeviceIdType.MESH
        )

    @pl.when((mine == 0) | (mine == last))
    def _():
        pl.semaphore_wait(barrier, shards)

    @pl.when((mine > 0) & (mine < last))
    def _():
        pl.semaphore_wait(barrier, shards + 1)

    def sum_copy(piece, slot):
        return pltpu.make_async_remote_copy(
            src_ref=stage_ref.at[piece],
            dst_ref=landed_ref.at[slot, piece],
            send_sem=sum_send.at[piece],
            recv_sem=sum_recv.at[slot, piece],
            device_id={"head": inward},
            device_id_type=pl.DeviceIdType.MESH,
        )

    def final_copy(piece):
        return pltpu.make_async_remote_copy(
            src_ref=final_ref.at[piece],
            dst_ref=final_ref.at[piece],
            send_sem=final_send.at[piece],
            recv_sem=final_recv.at[piece],
            device_id={"head": outward},
            device_id_type=pl.DeviceIdType.MESH,
        )

    def shard_copy(chunk, offset, source):
        start = pl.multiple_of(source * rows + chunk * piece_rows, 16)
        block = shared_ref.at[pl.ds(start, piece_rows)]
        return pltpu.make_async_remote_copy(
            src_ref=block,
            dst_ref=block,
            send_sem=shard_send.at[chunk, offset],
            recv_sem=shard_recv.at[chunk, offset],
            device_id={"seq": (shard + offset) % shards},
            device_id_type=pl.DeviceIdType.MESH,
        )

    def chunk_rows(chunk):
        return pl.ds(pl.multiple_of(chunk * piece_rows, 16), piece_rows)

    def compute(block):
        products = jnp.dot(
            normed_ref[...], block_weight_ref[block], preferred_element_type=jnp.float32
        )
        for chunk in range(chunks):
            here = slice(chunk * piece_rows, (chunk + 1) * piece_rows)
            partial_ref[chunk * blocks + block] = products[here]

        @pl.when(block // per_owner == mine)
        def _():
            columns = pl.ds(
                pl.multiple_of((block % per_owner) * piece_width, 128), piece_width
            )
            for chunk in range(chunks):
                here = slice(chunk * piece_rows, (chunk + 1) * piece_rows)
                partial_ref[chunk * blocks + block] += residual_ref[here, columns].astype(
                    jnp.float32
                )

        @pl.when(place == 0)
        def _():
            for chunk in range(chunks):
                piece = chunk * blocks + block
                stage_ref[piece] = partial_ref[piece].astype(jnp.bfloat16)
            sum_copy(block, inner_slot).start()

    def pass_inward(piece):
        @pl.when(place > 0)
        def _():
            sum_copy(piece, 0).wait_recv()
            arrived = landed_ref[0, piece].astype(jnp.float32)
            stage_ref[piece] = (partial_ref[piece] + arrived).astype(jnp.bfloat16)
            sum_copy(piece, inner_slot).start()

    def finish(piece):
        @pl.when(inner)
        def _():
            sum_copy(piece, 1).wait_recv()
            final_ref[piece] = (
                stage_ref[piece].astype(jnp.float32) + landed_ref[1, piece].astype(jnp.float32)
            ).astype(jnp.bfloat16)

        @pl.when(jnp.logical_not(inner))
        def _():
            final_copy(piece).wait_recv()

        @pl.when(place > 0)
        def _():
            final_copy(piece).start()

    def normalise(chunk):
        squares = jnp.zeros((piece_rows, 1), jnp.float32)
        for block in range(blocks):
            values = final_ref[chunk * blocks + block].astype(jnp.float32)
            squares += jnp.sum(values * values, axis=1, keepdims=True)
        scale = lax.rsqrt(squares / (count * width) + EPSILON)
        for block in range(blocks):
            columns = slice(block * piece_width, (block + 1) * piece_width)
            values = final_ref[chunk * blocks + block].astype(jnp.float32)
            attn_ref[:, columns] = (values * scale * gain_ref[:, columns]).astype(jnp.bfloat16)
        for part in range(per_owner):
            columns = slice(part * piece_width, (part + 1) * piece_width)
            layer_ref[chunk_rows(chunk), columns] = final_ref[
                chunk * blocks + mine * per_owner + part
            ]

    def product(index):
        columns = pl.ds(pl.multiple_of(index * tile, 128), tile)
        return jnp.dot(
            attn_ref[...], weight_ref[:, columns], preferred_element_type=jnp.float32
        ).astype(jnp.bfloat16)

    def project_shared(chunk):
        start = pl.multiple_of(shard * rows + chunk * piece_rows, 16)
        shared_ref[pl.ds(start, piece_rows)] = product(0)
        for offset in range(1, shards):

            @pl.when(shard + offset < shards)
            def _():
                shard_copy(chunk, offset, shard).start()

    def project_query(chunk, index):
        columns = pl.ds(pl.multiple_of(index * tile, 128), tile)
        query_ref[chunk_rows(chunk), columns] = product(index + 1)

    @pl.loop(0, blocks)
    def _(block):
        block_load(block).wait()
        compute(block)

    @pl.when(place == 0)
    def _():
        @pl.loop(blocks, pieces)
        def _(piece):
            sum_copy(piece, inner_slot).start()

    for other in range(shards):

        @pl.when(other > shard)
        def _():
            shared_ref[pl.ds(other * rows, rows)] = jnp.zeros((rows, tile), jnp.bfloat16)

    query_tiles = query_width // tile
    spacing = max(1, (blocks - 1) // (1 + query_tiles))
    first = lag + blocks - 1

    @pl.loop(0, pieces + lag + blocks - 1)
    def _(tick):
        @pl.when(tick < pieces)
        def _():
            pass_inward(tick)

        @pl.when((tick >= lag) & (tick < pieces + lag))
        def _():
            finish(tick - lag)

        @pl.when(tick == first)
        def _():
            for load in loads:
                load.wait()

        @pl.when(tick >= first)
        def _():
            chunk, turn = (tick - first) // blocks, (tick - first) % blocks

            @pl.when(turn == 0)
            def _():
                normalise(chunk)
                project_shared(chunk)

            @pl.when((turn > 0) & (turn % spacing == 0) & (turn // spacing <= query_tiles))
            def _():
                project_query(chunk, turn // spacing - 1)

    @pl.loop(0, pieces)
    def _(piece):
        sum_copy(piece, inner_slot).wait_send()

        @pl.when(place > 0)
        def _():
            final_copy(piece).wait_send()

    @pl.loop(0, chunks)
    def _(chunk):
        for offset in range(1, shards):

            @pl.when(shard + offset < shards)
            def _():
                shard_copy(chunk, offset, shard).wait_send()

            @pl.when(shard >= offset)
            def _():
                shard_copy(chunk, offset, shard - offset).wait_recv()

    key_value_ref[...] = shared_ref[...]


def line_layer(normed, out_weight, residual, norm_gain, weights, count, shards):
    rows, width = residual.shape
    model_width = width * count
    query_width, kv_width = weights[0].shape[1], weights[1].shape[1]
    piece_rows = 64 if rows % 64 == 0 else rows
    piece_width = 512 if width % 512 == 0 else width
    chunks, blocks = rows // piece_rows, model_width // piece_width
    pieces = chunks * blocks
    piece = (piece_rows, piece_width)
    lag = 3 * max(1, count - 3)
    vmem = pl.BlockSpec(memory_space=pltpu.VMEM)
    hbm = pl.BlockSpec(memory_space=pltpu.HBM)
    return pl.pallas_call(
        functools.partial(line_kernel, count, shards, chunks, lag),
        out_shape=(
            jax.ShapeDtypeStruct((rows, width), jnp.bfloat16),
            jax.ShapeDtypeStruct((rows, query_width), jnp.bfloat16),
            jax.ShapeDtypeStruct((shards * rows, 2 * kv_width), jnp.bfloat16),
        ),
        in_specs=[vmem, hbm, vmem, vmem, hbm, hbm, hbm],
        out_specs=[vmem] * 3,
        scratch_shapes=[
            pltpu.VMEM((blocks, out_weight.shape[0], piece_width), jnp.bfloat16),
            pltpu.VMEM((pieces,) + piece, jnp.float32),
            pltpu.VMEM((model_width, 2 * kv_width + query_width), jnp.bfloat16),
            pltpu.VMEM((piece_rows, model_width), jnp.bfloat16),
            pltpu.VMEM((shards * rows, 2 * kv_width), jnp.bfloat16),
            pltpu.VMEM((pieces,) + piece, jnp.bfloat16),
            pltpu.VMEM((2, pieces) + piece, jnp.bfloat16),
            pltpu.VMEM((pieces,) + piece, jnp.bfloat16),
            pltpu.SemaphoreType.DMA((pieces,)),
            pltpu.SemaphoreType.DMA((2, pieces)),
            pltpu.SemaphoreType.DMA((pieces,)),
            pltpu.SemaphoreType.DMA((pieces,)),
            pltpu.SemaphoreType.DMA((chunks, shards)),
            pltpu.SemaphoreType.DMA((chunks, shards)),
            pltpu.SemaphoreType.DMA((3,)),
            pltpu.SemaphoreType.DMA((blocks,)),
        ],
        compiler_params=pltpu.CompilerParams(
            collective_id=0, has_side_effects=True, vmem_limit_bytes=52 * 1024 * 1024
        ),
    )(normed, out_weight, residual, norm_gain.reshape(1, model_width), *weights)


def attention_kernel(group_size, limits_ref, query_ref, key_ref, value_ref, out_ref):
    rows, count = query_ref.shape[0], key_ref.shape[0]
    limit, first = limits_ref[0], limits_ref[1]
    key_pos = lax.broadcasted_iota(jnp.int32, (rows, count), 1)
    positions = first + lax.broadcasted_iota(jnp.int32, (rows, count), 0)
    allowed = (key_pos <= positions) & (key_pos < limit)
    live = first + lax.broadcasted_iota(jnp.int32, (rows, 1), 0) < limit
    for head in range(group_size):
        columns = slice(head * HEAD_DIM, (head + 1) * HEAD_DIM)
        scores = lax.dot_general(
            query_ref[:, columns],
            key_ref[...],
            (((1,), (1,)), ((), ())),
            preferred_element_type=jnp.float32,
        ) * HEAD_DIM ** (-0.5)
        masked = jnp.where(allowed, scores, NEG_BIG)
        weights = jnp.exp(masked - jnp.max(masked, axis=1, keepdims=True))
        total = jnp.sum(weights, axis=1, keepdims=True)
        accum = jnp.dot(
            weights.astype(jnp.bfloat16), value_ref[...], preferred_element_type=jnp.float32
        )
        head_out = jnp.where(live, accum / jnp.where(live, total, 1.0), 0.0)
        out_ref[:, columns] = head_out.astype(jnp.bfloat16)


def attention(queries, key_value, limit, first):
    rows, count = queries.shape[0], key_value.shape[0]
    kv_local = key_value.shape[1] // (2 * HEAD_DIM)
    group_size = queries.shape[1] // (kv_local * HEAD_DIM)
    wide = (rows, group_size * HEAD_DIM)
    return pl.pallas_call(
        functools.partial(attention_kernel, group_size),
        grid=(kv_local,),
        out_shape=jax.ShapeDtypeStruct(queries.shape, jnp.bfloat16),
        in_specs=[
            pl.BlockSpec(memory_space=pltpu.SMEM),
            pl.BlockSpec(wide, lambda head: (0, head)),
            pl.BlockSpec((count, HEAD_DIM), lambda head: (0, head)),
            pl.BlockSpec((count, HEAD_DIM), lambda head: (0, head + kv_local)),
        ],
        out_specs=pl.BlockSpec(wide, lambda head: (0, head)),
        compiler_params=pltpu.CompilerParams(vmem_limit_bytes=40 * 1024 * 1024),
        cost_estimate=pl.CostEstimate(
            flops=4 * rows * count * queries.shape[1],
            bytes_accessed=4 * queries.size + 2 * key_value.size,
            transcendentals=rows * count * kv_local * group_size,
        ),
    )(jnp.stack([limit, first]), queries, key_value, key_value)


def body(
    length,
    residual,
    ssm_input,
    state_in,
    state_out,
    step_raw,
    decay_rate,
    ssm_gain,
    out_weight,
    norm_gain,
    query_weight,
    key_weight,
    value_weight,
):
    rows = residual.shape[0]
    local_heads = decay_rate.shape[0]
    head_width = ssm_input.shape[1] // local_heads
    seq_index = lax.axis_index("seq")
    limit = length[0]
    positions = seq_index * rows + jnp.arange(rows, dtype=jnp.int32)
    live_rows = positions < limit
    live = live_rows.astype(jnp.float32)
    delta = live[None, :] * jax.nn.softplus(step_raw)
    cumlog = jnp.cumsum(-decay_rate[:, None] * delta, axis=1)
    inputs = ssm_input.astype(jnp.float32).reshape(rows, local_heads, head_width)
    inner = jnp.dot(state_out, state_in.T, preferred_element_type=jnp.float32)
    causal = jnp.arange(rows)[:, None] >= jnp.arange(rows)[None, :]
    spread = cumlog[:, :, None] - cumlog[:, None, :]
    mixing = (
        jnp.where(causal[None], jnp.exp(jnp.where(causal[None], spread, 0.0)), 0.0)
        * inner[None]
        * delta[:, None, :]
    )
    within = jnp.einsum("hts,shp->thp", mixing, inputs, precision=HIGHEST)
    tail = jnp.exp(cumlog[:, -1:] - cumlog) * delta
    local_state = jnp.einsum(
        "hs,shp,sn->hpn", tail, inputs, state_in.astype(jnp.float32), precision=HIGHEST
    )
    incoming = incoming_state(jnp.exp(cumlog[:, -1]), local_state, lax.axis_size("seq"))
    carried = jnp.einsum("hpn,tn->thp", incoming, state_out.astype(jnp.float32), precision=HIGHEST)
    ssm_out = (within + jnp.exp(cumlog).T[:, :, None] * carried) * live[:, None, None]
    mean_square = jnp.mean(ssm_out * ssm_out, axis=2, keepdims=True)
    normed = (
        ssm_out * lax.rsqrt(mean_square + EPSILON) * ssm_gain.reshape(local_heads, head_width)
    ).astype(jnp.bfloat16)
    normed = normed.reshape(rows, local_heads * head_width)
    layer_out, queries, key_value = line_layer(
        normed,
        out_weight,
        residual,
        norm_gain,
        (query_weight, key_weight, value_weight),
        lax.axis_size("head"),
        lax.axis_size("seq"),
    )
    head_out = attention(queries, key_value, limit, seq_index * rows)
    return (layer_out, head_out)


def solution(mesh):
    placed = (
        P("doc"),
        P(("doc", "seq"), "head"),
        P(("doc", "seq"), "head"),
        P(("doc", "seq"), None),
        P(("doc", "seq"), None),
        P(("doc", "head"), "seq"),
        P("head"),
        P("head"),
        P("head", None),
        P(),
        P(None, "head"),
        P(None, "head"),
        P(None, "head"),
    )
    return jax.shard_map(
        body,
        mesh=mesh,
        in_specs=placed,
        out_specs=(P(("doc", "seq"), "head"), P(("doc", "seq"), "head")),
        check_vma=False,
    )
```
